32 devices in a mesh: expert: 4 (over x, core), shard: 8 (over z, y).
Axes of the slice: x: 2, y: 2, z: 4, core: 2. Of those that a mesh axis runs over, the one named last changes fastest.
Arguments:
- w_gate: float32 [64, 2048, 1408], P('expert', 'shard'), may hold values from -0.1875 to 0.1875
- w_up: float32 [64, 2048, 1408], P('expert', 'shard'), may hold values from -0.1875 to 0.1875
- router_weight: float32 [2048, 64], P('shard', 'expert'), may hold values from -0.125 to 0.125
- router_gain: float32 [2048], P('shard'), may hold values from 0.25 to 1.75
Outputs:
- serve_gate: bfloat16 [64, 2048, 1408], P('expert', None, 'shard')
- serve_up: bfloat16 [64, 2048, 1408], P('expert', None, 'shard')
- scale_gate: float32 [64, 1408], P('expert', 'shard')
- scale_up: float32 [64, 1408], P('expert', 'shard')
- serve_router: bfloat16 [2048, 64], replicated
The draws below stay inside these ranges and needn't reach their ends.
All inputs are finite; a program needn't handle non-finite values. Where the reference program divides by a largest or mean magnitude, that divisor is 1e-20 or more.
Results may differ from the reference program's by a relative error of at most 0.001.
Values may be sent and summed in bfloat16 or wider, within the bound.
A program may use at most 192 MiB of HBM per device.

```python
import jax
import jax.numpy as jnp

EXPERTS = 64
D_MODEL = 2048
D_EXPERT = 1408


def raised(result, key, source, target, parts, factor):
    owner, partner = [(jnp.arange(result.shape[dim]) // (result.shape[dim] // parts)).reshape([-1 if axis == dim else 1 for axis in range(result.ndim)]) for dim in (source, target)]
    chosen = jax.random.permutation(key, parts)[partner]
    strong = (owner == chosen) | (owner == (partner + parts // 2) % parts)
    return jnp.where(strong, factor * result, result)


def block_levels(rng, shape, split, least, high):
    factor_of, own = 1.0, jax.random.fold_in(rng, 6)
    for position, parts in split:
        draws = jnp.exp(jax.random.uniform(jax.random.fold_in(own, position), (parts,), jnp.float32, least / len(split), high / len(split)))
        factor_of = factor_of * jnp.repeat(draws, shape[position] // parts).reshape([-1 if axis == position else 1 for axis in range(len(shape))])
    return factor_of


def normal_values(stream_key, extent, spread, most, cuts=(), dtype=jnp.bfloat16):
    values = jax.random.normal(stream_key, extent, jnp.float32) * spread
    if len(cuts) > 0:
        values = block_levels(stream_key, extent, cuts, -0.22, 0.18) * values
    return jnp.clip(values, min=-most, max=most).astype(dtype)


def gaussian_with(stream_key, shape, deviation, limit, shards, heavy, held_as=jnp.bfloat16):
    entries = deviation * jax.random.normal(stream_key, shape, jnp.float32)
    if shards:
        entries = entries * block_levels(stream_key, shape, shards, -0.22, 0.18)
    return jnp.clip(raised(entries, jax.random.fold_in(stream_key, 3), *heavy), -limit, limit).astype(held_as)


def setup_inputs(seed: int = 0) -> dict:
    key_list = jax.random.split(jax.random.key(seed), 5)
    return {
        "w_gate": gaussian_with(key_list[0], (EXPERTS, D_MODEL, D_EXPERT), D_MODEL ** -0.5, 0.1875, ((0, 4), (1, 8)), (1, 2, 8, 2.0), jnp.float32),
        "w_up": gaussian_with(key_list[1], (EXPERTS, D_MODEL, D_EXPERT), D_MODEL ** -0.5, 0.1875, ((0, 4), (1, 8)), (1, 2, 8, 2.0), jnp.float32),
        "router_weight": normal_values(key_list[2], (D_MODEL, EXPERTS), D_MODEL ** -0.5, 0.125, ((0, 8), (1, 4)), jnp.float32),
        "router_gain": jnp.clip(1.0 + 0.15 * jax.random.normal(key_list[3], (D_MODEL,), jnp.float32), 0.25, 1.75),
    }


def reference(w_gate, w_up, router_weight, router_gain):
    scale_gate = jnp.sum(jnp.abs(w_gate), axis=1) / D_MODEL
    serve_gate = (w_gate / jnp.expand_dims(scale_gate, 1)).astype(jnp.bfloat16)
    scale_up = jnp.sum(jnp.abs(w_up), axis=1) / D_MODEL
    serve_up = (w_up / jnp.expand_dims(scale_up, 1)).astype(jnp.bfloat16)
    serve_router = (router_weight * router_gain[:, None]).astype(jnp.bfloat16)
    return serve_gate, serve_up, scale_gate, scale_up, serve_router
```

```python
import functools

import jax
import jax.numpy as jnp
from jax import lax
from jax.experimental import pallas as pl
from jax.experimental.pallas import tpu as pltpu
from jax.sharding import PartitionSpec as P

LANES = 128
SLOTS = 4
EARLY = 3
AHEAD = 12


def plain(w_gate, w_up, router_weight, router_gain):
    model = w_gate.shape[1] * lax.axis_size("shard")
    total_gate, total_up = lax.psum(
        (jnp.sum(jnp.abs(w_gate), axis=1), jnp.sum(jnp.abs(w_up), axis=1)), "shard"
    )
    served = []
    scales = []
    for w, total in ((w_gate, total_gate), (w_up, total_up)):
        scale = total / model
        narrow = (w / jnp.expand_dims(scale, 1)).astype(jnp.bfloat16)
        out = lax.all_to_all(narrow, "shard", split_axis=2, concat_axis=1, tiled=True)
        served.append(out)
        scales.append(
            lax.dynamic_slice_in_dim(
                scale, lax.axis_index("shard") * out.shape[2], out.shape[2], axis=1
            )
        )
    part_router = (router_weight * router_gain[:, None]).astype(jnp.bfloat16)
    row_router = lax.all_gather(part_router, "shard", axis=0, tiled=True)
    serve_router = lax.all_gather(row_router, "expert", axis=1, tiled=True)
    return (*served, *scales, serve_router)


def kernel(
    n, groups, model,
    weight_ref, gain_ref, gate_ref, up_ref,
    out_gate, out_up, scale_ref, out_router,
    stage, kept, loaded, part, quick, first, near_sum, far_sum, half_sum, raw, gains,
    load_sem, kept_sem, raw_sem, early_send, early_recv,
    near_send, near_recv, far_send, far_recv, mean_send, mean_recv,
    row_send, row_recv, col_send, col_recv, data_send, data_recv,
):
    me = lax.axis_index("shard")
    group = lax.axis_index("expert")
    experts, rows, width = gate_ref.shape
    tasks, tiles, _ = part.shape
    half = n // 2
    share = tasks // half
    columns = width // n
    heads = weight_ref.shape[0]
    later = tasks - EARLY
    side, spot = me // half, lax.rem(me, half)

    def sent_to(i):
        if i < half:
            return (1 - side) * half + lax.rem(spot + i, half)
        return side * half + lax.rem(spot + i - half + 1, half)

    def come_from(i):
        if i < half:
            return (1 - side) * half + lax.rem(spot + half - i, half)
        return side * half + lax.rem(spot + half - (i - half + 1), half)

    peers = range(n - 1)
    near = range(half, n - 1)

    def remote(src, dst, send, recv, shard=None, expert=None):
        return pltpu.make_async_remote_copy(
            src_ref=src, dst_ref=dst, send_sem=send, recv_sem=recv,
            device_id={"shard": shard} if expert is None else {"expert": expert},
        )

    def start_load(j):
        task, slot = EARLY + lax.rem(j, later), lax.rem(j, SLOTS)

        @pl.when((j < 2 * later) & (task < experts))
        def _():
            pltpu.make_async_copy(
                gate_ref.at[task], loaded.at[slot], load_sem.at[slot]
            ).start()

        @pl.when((j < 2 * later) & (task >= experts))
        def _():
            pltpu.make_async_copy(
                up_ref.at[task - experts], loaded.at[slot], load_sem.at[slot]
            ).start()

    def wait_load(slot):
        pltpu.make_async_copy(
            gate_ref.at[0], loaded.at[slot], load_sem.at[slot]
        ).wait()

    def keep(task):
        return pltpu.make_async_copy(
            gate_ref.at[task], kept.at[task], kept_sem.at[task]
        )

    def add_up(task, ref, slot):
        for t in range(tiles):
            lanes = slice(t * LANES, (t + 1) * LANES)
            part[task, t : t + 1, :] = jnp.sum(
                jnp.abs(ref[slot, :, lanes]), axis=0, keepdims=True
            )

    def add_later(j, carry):
        slot = lax.rem(j, SLOTS)
        wait_load(slot)
        add_up(EARLY + j, loaded, slot)
        start_load(j + SLOTS)
        return carry

    def shape_task(task, ref, slot, means, index):
        for t in range(tiles):
            lanes = slice(t * LANES, (t + 1) * LANES)
            inverse = 1.0 / means[index, t : t + 1, :]
            scaled = ref[slot, :, lanes] * inverse
            stage[task, lanes, :] = scaled.T.astype(jnp.bfloat16)

    my_rows = pl.ds(pl.multiple_of(me * rows, rows), rows)

    def piece(k):
        return pl.ds(pl.multiple_of(k * columns, 16), columns)

    def send_task(task, w, out, chosen):
        e = task - w * experts
        for i in chosen:
            remote(
                stage.at[task, piece(sent_to(i))],
                out.at[e, :, my_rows],
                data_send.at[w, i],
                data_recv.at[w, i],
                shard=sent_to(i),
            ).start()

    def keep_own(task, w, out):
        out[task - w * experts, :, my_rows] = stage[task, piece(me)]

    for task in range(EARLY):
        keep(task).start()
    fetch_weight = pltpu.make_async_copy(weight_ref, raw, raw_sem.at[0])
    fetch_gain = pltpu.make_async_copy(gain_ref, gains, raw_sem.at[1])
    fetch_weight.start()
    fetch_gain.start()
    for j in range(SLOTS):
        start_load(j)

    barrier = pltpu.get_barrier_semaphore()
    for i in peers:
        pl.semaphore_signal(barrier, inc=1, device_id={"shard": sent_to(i)})
    for q in range(1, groups):
        pl.semaphore_signal(
            barrier, inc=1, device_id={"expert": lax.rem(group + q, groups)}
        )

    started = []

    def begin(copy):
        copy.start()
        started.append(copy)
        return copy

    keep(0).wait()
    add_up(0, kept, 0)
    pl.semaphore_wait(barrier, n - 1 + groups - 1)

    early = []
    for i in peers:
        early.append(begin(remote(
            part.at[pl.ds(0, 1)], first.at[me, pl.ds(0, 1)],
            early_send.at[0, i], early_recv.at[0, i], shard=sent_to(i),
        )))
    first[me, 0:1] = part[0:1]
    for task in range(1, EARLY):
        keep(task).wait()
        add_up(task, kept, task)
    rest = []
    for i in peers:
        rest.append(begin(remote(
            part.at[pl.ds(1, EARLY - 1)], first.at[me, pl.ds(1, EARLY - 1)],
            early_send.at[1, i], early_recv.at[1, i], shard=sent_to(i),
        )))
    first[me, 1:EARLY] = part[1:EARLY]

    fetch_weight.wait()
    fetch_gain.wait()
    mine = pl.ds(pl.multiple_of(group * heads, heads), heads)
    out_router[mine, my_rows] = (raw[...] * gains[...]).astype(jnp.bfloat16)
    lines = []
    for i in peers:
        lines.append(begin(remote(
            out_router.at[mine, my_rows], out_router.at[mine, my_rows],
            row_send.at[i], row_recv.at[i], shard=sent_to(i),
        )))

    lax.fori_loop(0, AHEAD, add_later, 0)

    def early_mean(lo, hi):
        total = first[0, lo:hi]
        for s in range(1, n):
            total = total + first[s, lo:hi]
        quick[lo:hi] = total / model

    for copy in early:
        copy.wait_recv()
    early_mean(0, 1)
    shape_task(0, kept, 0, quick, 0)
    send_task(0, 0, out_gate, peers)

    lax.fori_loop(AHEAD, later, add_later, 0)

    sums = []
    for i in near:
        sums.append(begin(remote(
            part.at[pl.ds(sent_to(i) % half * share, share)],
            near_sum.at[i - half],
            near_send.at[i - half], near_recv.at[i - half], shard=sent_to(i),
        )))
    keep_own(0, 0, out_gate)
    for copy in rest:
        copy.wait_recv()
    early_mean(1, EARLY)
    shape_task(1, kept, 1, quick, 1)
    send_task(1, 0, out_gate, range(half // 2))

    own = pl.ds(spot * share, share)
    total = part[own]
    for i, copy in zip(near, sums):
        copy.wait_recv()
        total = total + near_sum[i - half]
    half_sum[...] = total
    across = begin(remote(
        half_sum, far_sum, far_send, far_recv, shard=sent_to(0)
    ))
    send_task(1, 0, out_gate, range(half // 2, n - 1))
    keep_own(1, 0, out_gate)

    for task in range(2, EARLY):
        shape_task(task, kept, task, quick, task)
    across.wait_recv()
    scale_ref[own] = (half_sum[...] + far_sum[...]) / model
    means = []
    for i in near:
        means.append(begin(remote(
            scale_ref.at[own], scale_ref.at[own],
            mean_send.at[i - half], mean_recv.at[i - half], shard=sent_to(i),
        )))
    for task in range(2, EARLY):
        send_task(task, 0, out_gate, peers)
        keep_own(task, 0, out_gate)

    for copy in lines:
        copy.wait_recv()
    cols = []
    for q in range(1, groups):
        cols.append(begin(remote(
            out_router.at[mine], out_router.at[mine],
            col_send.at[q], col_recv.at[q], expert=lax.rem(group + q, groups),
        )))
    for copy in means:
        copy.wait_recv()

    for w, out in enumerate((out_gate, out_up)):

        def step(task, carry, w=w, out=out):
            j = later + task - EARLY
            slot = lax.rem(j, SLOTS)
            wait_load(slot)
            shape_task(task, loaded, slot, scale_ref, task)
            send_task(task, w, out, peers)
            keep_own(task, w, out)
            start_load(j + SLOTS)
            return carry

        lax.fori_loop(max(EARLY, w * experts), (w + 1) * experts, step, 0)

    for copy in cols:
        copy.wait_recv()
    for copy in started:
        copy.wait_send()
    for w, out in enumerate((out_gate, out_up)):
        held = pl.ds(w * experts, experts)
        for i in peers:
            from_i = pl.ds(pl.multiple_of(come_from(i) * rows, rows), rows)
            both = remote(
                stage.at[held, piece(sent_to(i))], out.at[:, :, from_i],
                data_send.at[w, i], data_recv.at[w, i], shard=sent_to(i),
            )
            both.wait_send()
            both.wait_recv()


def settle(count, *refs):
    sources, outs, sem = refs[:count], refs[count : 2 * count], refs[-1]
    copies = [
        pltpu.make_async_copy(src, dst, sem.at[i])
        for i, (src, dst) in enumerate(zip(sources, outs))
    ]
    for copy in copies:
        copy.start()
    for copy in copies:
        copy.wait()


def on_device(w_gate, w_up, router_weight, router_gain):
    n, groups = lax.axis_size("shard"), lax.axis_size("expert")
    experts, rows, width = w_gate.shape
    heads = router_weight.shape[1]
    tasks, columns, model = 2 * experts, width // n, rows * n
    if (
        n % 2
        or n < 4
        or rows % LANES
        or width % LANES
        or columns % 16
        or heads % 16
        or tasks % (n // 2)
        or experts < EARLY + AHEAD
    ):
        return plain(w_gate, w_up, router_weight, router_gain)
    tiles, half = width // LANES, n // 2
    share = tasks // half
    hbm = pl.BlockSpec(memory_space=pl.ANY)
    vmem = pl.BlockSpec(memory_space=pltpu.VMEM)
    dma = pltpu.SemaphoreType.DMA
    held = (
        ((experts, columns, model), jnp.bfloat16),
        ((experts, columns, model), jnp.bfloat16),
        ((tasks, tiles, LANES), jnp.float32),
        ((heads * groups, model), jnp.bfloat16),
    )
    block = (share, tiles, LANES)
    arrived = pl.pallas_call(
        functools.partial(kernel, n, groups, model),
        out_shape=tuple(pltpu.VMEM(*a) for a in held),
        in_specs=[hbm] * 4,
        out_specs=(vmem,) * 4,
        scratch_shapes=[
            pltpu.VMEM((tasks, width, rows), jnp.bfloat16),
            pltpu.VMEM((EARLY, rows, width), jnp.float32),
            pltpu.VMEM((SLOTS, rows, width), jnp.float32),
            pltpu.VMEM((tasks, tiles, LANES), jnp.float32),
            pltpu.VMEM((EARLY, tiles, LANES), jnp.float32),
            pltpu.VMEM((n, EARLY, tiles, LANES), jnp.float32),
            pltpu.VMEM((half - 1, *block), jnp.float32),
            pltpu.VMEM(block, jnp.float32),
            pltpu.VMEM(block, jnp.float32),
            pltpu.VMEM((heads, rows), jnp.float32),
            pltpu.VMEM((1, rows), jnp.float32),
            dma((SLOTS,)), dma((EARLY,)), dma((2,)),
            dma((2, n - 1)), dma((2, n - 1)),
            dma((half - 1,)), dma((half - 1,)),
            dma, dma,
            dma((half - 1,)), dma((half - 1,)),
            dma((n - 1,)), dma((n - 1,)),
            dma((groups,)), dma((groups,)),
            dma((2, n - 1)), dma((2, n - 1)),
        ],
        compiler_params=pltpu.CompilerParams(
            collective_id=0, has_side_effects=True, vmem_limit_bytes=38 * 2**20
        ),
    )(router_weight.T, router_gain[None, :], w_gate, w_up)
    out_gate, out_up, scale, router = pl.pallas_call(
        functools.partial(settle, len(held)),
        out_shape=tuple(jax.ShapeDtypeStruct(*a) for a in held),
        in_specs=[vmem] * len(held),
        out_specs=(hbm,) * len(held),
        scratch_shapes=[dma((len(held),))],
        compiler_params=pltpu.CompilerParams(vmem_limit_bytes=2**20),
    )(*arrived)
    mine = lax.dynamic_slice_in_dim(
        scale.reshape(tasks, width), lax.axis_index("shard") * columns, columns, axis=1
    )
    return (
        out_gate.swapaxes(1, 2),
        out_up.swapaxes(1, 2),
        mine[:experts],
        mine[experts:],
        router.T,
    )


def solution(mesh):
    placed = (
        P("expert", "shard", None),
        P("expert", "shard", None),
        P("shard", "expert"),
        P("shard"),
    )
    return jax.shard_map(
        on_device,
        mesh=mesh,
        in_specs=placed,
        out_specs=(
            P("expert", None, "shard"),
            P("expert", None, "shard"),
            P("expert", "shard"),
            P("expert", "shard"),
            P(),
        ),
        check_vma=False,
    )
```

```python
import functools

import jax
import jax.numpy as jnp
from jax import lax
from jax.experimental import pallas as pl
from jax.experimental.pallas import tpu as pltpu
from jax.sharding import PartitionSpec as P

LANES = 128
SLOTS = 4
EARLY = 3
AHEAD = 2
PARTS = 8
LEAD = 3


def plain(w_gate, w_up, router_weight, router_gain):
    model = w_gate.shape[1] * lax.axis_size("shard")
    total_gate, total_up = lax.psum(
        (jnp.sum(jnp.abs(w_gate), axis=1), jnp.sum(jnp.abs(w_up), axis=1)), "shard"
    )
    served = []
    scales = []
    for w, total in ((w_gate, total_gate), (w_up, total_up)):
        scale = total / model
        narrow = (w / jnp.expand_dims(scale, 1)).astype(jnp.bfloat16)
        out = lax.all_to_all(narrow, "shard", split_axis=2, concat_axis=1, tiled=True)
        served.append(out)
        scales.append(
            lax.dynamic_slice_in_dim(
                scale, lax.axis_index("shard") * out.shape[2], out.shape[2], axis=1
            )
        )
    part_router = (router_weight * router_gain[:, None]).astype(jnp.bfloat16)
    row_router = lax.all_gather(part_router, "shard", axis=0, tiled=True)
    serve_router = lax.all_gather(row_router, "expert", axis=1, tiled=True)
    return (*served, *scales, serve_router)


def kernel(
    n, groups, model,
    weight_ref, gain_ref, gate_ref, up_ref,
    out_gate, out_up, gate_scale, up_scale, out_router,
    scale_ref, stage, kept, loaded, part, quick, first, near_sum, far_sum, half_sum, raw, gains,
    load_sem, kept_sem, raw_sem, early_send, early_recv,
    near_send, near_recv, far_send, far_recv, mean_send, mean_recv,
    row_send, row_recv, col_send, col_recv, data_send, data_recv,
):
    me = lax.axis_index("shard")
    group = lax.axis_index("expert")
    experts, rows, width = gate_ref.shape
    tasks, tiles, _ = part.shape
    half = n // 2
    share = tasks // half
    columns = width // n
    heads = weight_ref.shape[0]
    later = tasks - EARLY
    side, spot = me // half, lax.rem(me, half)

    peers = range(n - 1)
    near = range(half - 1)

    def sent_to(i):
        return lax.rem(me + i + 1, n)

    def come_from(i):
        return lax.rem(me + n - i - 1, n)

    def beside(i):
        return side * half + lax.rem(spot + i + 1, half)

    across = lax.rem(me + half, n)

    def remote(src, dst, send, recv, shard=None, expert=None):
        return pltpu.make_async_remote_copy(
            src_ref=src, dst_ref=dst, send_sem=send, recv_sem=recv,
            device_id={"shard": shard} if expert is None else {"expert": expert},
        )

    def start_load(j):
        task, slot = EARLY + lax.rem(j, later), lax.rem(j, SLOTS)

        @pl.when((j < 2 * later) & (task < experts))
        def _():
            pltpu.make_async_copy(
                gate_ref.at[task], loaded.at[slot], load_sem.at[slot]
            ).start()

        @pl.when((j < 2 * later) & (task >= experts))
        def _():
            pltpu.make_async_copy(
                up_ref.at[task - experts], loaded.at[slot], load_sem.at[slot]
            ).start()

    def wait_load(slot):
        pltpu.make_async_copy(
            gate_ref.at[0], loaded.at[slot], load_sem.at[slot]
        ).wait()

    def keep(task):
        return pltpu.make_async_copy(
            gate_ref.at[task], kept.at[task], kept_sem.at[task]
        )

    def add_up(task, ref, slot):
        for t in range(tiles):
            lanes = slice(t * LANES, (t + 1) * LANES)
            part[task, t : t + 1, :] = jnp.sum(
                jnp.abs(ref[slot, :, lanes]), axis=0, keepdims=True
            )

    def add_later(j, carry):
        slot = lax.rem(j, SLOTS)
        wait_load(slot)
        add_up(EARLY + j, loaded, slot)
        start_load(j + SLOTS)
        return carry

    def shape_task(task, ref, slot, means, index):
        for t in range(tiles):
            lanes = slice(t * LANES, (t + 1) * LANES)
            inverse = 1.0 / means[index, t : t + 1, :]
            scaled = ref[slot, :, lanes] * inverse
            stage[task, lanes, :] = scaled.T.astype(jnp.bfloat16)

    my_rows = pl.ds(pl.multiple_of(me * rows, rows), rows)

    def piece(k):
        return pl.ds(pl.multiple_of(k * columns, 16), columns)

    def send_task(task, w, out, chosen):
        e = task - w * experts
        for i in chosen:
            remote(
                stage.at[task, piece(sent_to(i))],
                out.at[e, :, my_rows],
                data_send.at[w, i],
                data_recv.at[w, i],
                shard=sent_to(i),
            ).start()

    def keep_own(task, w, out):
        out[task - w * experts, :, my_rows] = stage[task, piece(me)]

    for task in range(EARLY):
        keep(task).start()
    fetch_weight = pltpu.make_async_copy(weight_ref, raw, raw_sem.at[0])
    fetch_gain = pltpu.make_async_copy(gain_ref, gains, raw_sem.at[1])
    fetch_weight.start()
    fetch_gain.start()
    for j in range(SLOTS):
        start_load(j)

    barrier = pltpu.get_barrier_semaphore()
    for i in peers:
        pl.semaphore_signal(barrier, inc=1, device_id={"shard": sent_to(i)})
    for q in range(1, groups):
        pl.semaphore_signal(
            barrier, inc=1, device_id={"expert": lax.rem(group + q, groups)}
        )

    started = []

    def begin(copy):
        copy.start()
        started.append(copy)
        return copy

    keep(0).wait()
    add_up(0, kept, 0)
    pl.semaphore_wait(barrier, n - 1 + groups - 1)

    early = []
    for i in peers:
        early.append(begin(remote(
            part.at[pl.ds(0, 1)], first.at[me, pl.ds(0, 1)],
            early_send.at[0, i], early_recv.at[0, i], shard=sent_to(i),
        )))
    first[me, 0:1] = part[0:1]
    for task in range(1, EARLY):
        keep(task).wait()
        add_up(task, kept, task)
    rest = []
    for i in peers:
        rest.append(begin(remote(
            part.at[pl.ds(1, EARLY - 1)], first.at[me, pl.ds(1, EARLY - 1)],
            early_send.at[1, i], early_recv.at[1, i], shard=sent_to(i),
        )))
    first[me, 1:EARLY] = part[1:EARLY]

    fetch_weight.wait()
    fetch_gain.wait()
    mine = pl.ds(pl.multiple_of(group * heads, heads), heads)
    out_router[mine, my_rows] = (raw[...] * gains[...]).astype(jnp.bfloat16)
    lines = []
    for i in peers:
        lines.append(begin(remote(
            out_router.at[mine, my_rows], out_router.at[mine, my_rows],
            row_send.at[i], row_recv.at[i], shard=sent_to(i),
        )))

    lax.fori_loop(0, AHEAD, add_later, 0)

    def early_mean(lo, hi):
        total = first[0, lo:hi]
        for s in range(1, n):
            total = total + first[s, lo:hi]
        quick[lo:hi] = total / model

    for copy in early:
        copy.wait_recv()
    early_mean(0, 1)
    shape_task(0, kept, 0, quick, 0)
    send_task(0, 0, out_gate, peers)

    lax.fori_loop(AHEAD, later, add_later, 0)

    sums = []
    for i in near:
        sums.append(begin(remote(
            part.at[pl.ds(lax.rem(beside(i), half) * share, share)],
            near_sum.at[i], near_send.at[i], near_recv.at[i], shard=beside(i),
        )))
    keep_own(0, 0, out_gate)
    for copy in rest:
        copy.wait_recv()
    early_mean(1, EARLY)
    shape_task(1, kept, 1, quick, 1)
    send_task(1, 0, out_gate, range(LEAD))

    own = pl.ds(spot * share, share)
    total = part[own]
    for i, copy in zip(near, sums):
        copy.wait_recv()
        total = total + near_sum[i]
    half_sum[...] = total
    crossing = begin(remote(half_sum, far_sum, far_send, far_recv, shard=across))
    send_task(1, 0, out_gate, range(LEAD, n - 1))
    keep_own(1, 0, out_gate)

    for task in range(2, EARLY):
        shape_task(task, kept, task, quick, task)
    crossing.wait_recv()
    scale_ref[own] = (half_sum[...] + far_sum[...]) / model
    means = []
    for i in near:
        means.append(begin(remote(
            scale_ref.at[own], scale_ref.at[own],
            mean_send.at[i], mean_recv.at[i], shard=beside(i),
        )))
    for task in range(2, EARLY):
        send_task(task, 0, out_gate, peers)
        keep_own(task, 0, out_gate)

    for copy in lines:
        copy.wait_recv()
    cols = []
    for q in range(1, groups):
        cols.append(begin(remote(
            out_router.at[mine], out_router.at[mine],
            col_send.at[q], col_recv.at[q], expert=lax.rem(group + q, groups),
        )))
    for copy in means:
        copy.wait_recv()

    for k in range(n):

        @pl.when(me == k)
        def _(k=k):
            lo = k * columns
            for t in range(lo // LANES, (lo + columns - 1) // LANES + 1):
                left = max(lo, t * LANES)
                right = min(lo + columns, (t + 1) * LANES)
                seen = scale_ref[:, t, left - t * LANES : right - t * LANES]
                gate_scale[:, left - lo : right - lo] = seen[:experts]
                up_scale[:, left - lo : right - lo] = seen[experts:]

    for w, out in enumerate((out_gate, out_up)):

        def step(task, carry, w=w, out=out):
            j = later + task - EARLY
            slot = lax.rem(j, SLOTS)
            wait_load(slot)
            shape_task(task, loaded, slot, scale_ref, task)
            send_task(task, w, out, peers)
            keep_own(task, w, out)
            start_load(j + SLOTS)
            return carry

        lax.fori_loop(max(EARLY, w * experts), (w + 1) * experts, step, 0)

    for copy in cols:
        copy.wait_recv()
    for copy in started:
        copy.wait_send()
    for w, out in enumerate((out_gate, out_up)):
        held = pl.ds(w * experts, experts)
        for i in peers:
            from_i = pl.ds(pl.multiple_of(come_from(i) * rows, rows), rows)
            both = remote(
                stage.at[held, piece(sent_to(i))], out.at[:, :, from_i],
                data_send.at[w, i], data_recv.at[w, i], shard=sent_to(i),
            )
            both.wait_send()
            both.wait_recv()


def settle(count, *refs):
    sources, outs, sem = refs[:count], refs[count : 2 * count], refs[-1]
    copies = []
    for i, (src, dst) in enumerate(zip(sources, outs)):
        parts = PARTS if src.ndim == 3 and src.shape[0] % PARTS == 0 else 1
        step = src.shape[0] // parts
        for k in range(parts):
            rows = pl.ds(k * step, step)
            copies.append(
                pltpu.make_async_copy(src.at[rows], dst.at[rows], sem.at[i, k])
            )
    for copy in copies:
        copy.start()
    for copy in copies:
        copy.wait()


def on_device(w_gate, w_up, router_weight, router_gain):
    n, groups = lax.axis_size("shard"), lax.axis_size("expert")
    experts, rows, width = w_gate.shape
    heads = router_weight.shape[1]
    tasks, columns, model = 2 * experts, width // n, rows * n
    if (
        n % 2
        or n < 4
        or rows % LANES
        or width % LANES
        or columns % 16
        or heads % 16
        or tasks % (n // 2)
        or experts < EARLY + AHEAD
    ):
        return plain(w_gate, w_up, router_weight, router_gain)
    tiles, half = width // LANES, n // 2
    share = tasks // half
    hbm = pl.BlockSpec(memory_space=pl.ANY)
    vmem = pl.BlockSpec(memory_space=pltpu.VMEM)
    dma = pltpu.SemaphoreType.DMA
    held = (
        ((experts, columns, model), jnp.bfloat16),
        ((experts, columns, model), jnp.bfloat16),
        ((experts, columns), jnp.float32),
        ((experts, columns), jnp.float32),
        ((heads * groups, model), jnp.bfloat16),
    )
    block = (share, tiles, LANES)
    arrived = pl.pallas_call(
        functools.partial(kernel, n, groups, model),
        out_shape=tuple(pltpu.VMEM(*a) for a in held),
        in_specs=[hbm] * 4,
        out_specs=(vmem,) * len(held),
        scratch_shapes=[
            pltpu.VMEM((tasks, tiles, LANES), jnp.float32),
            pltpu.VMEM((tasks, width, rows), jnp.bfloat16),
            pltpu.VMEM((EARLY, rows, width), jnp.float32),
            pltpu.VMEM((SLOTS, rows, width), jnp.float32),
            pltpu.VMEM((tasks, tiles, LANES), jnp.float32),
            pltpu.VMEM((EARLY, tiles, LANES), jnp.float32),
            pltpu.VMEM((n, EARLY, tiles, LANES), jnp.float32),
            pltpu.VMEM((half - 1, *block), jnp.float32),
            pltpu.VMEM(block, jnp.float32),
            pltpu.VMEM(block, jnp.float32),
            pltpu.VMEM((heads, rows), jnp.float32),
            pltpu.VMEM((1, rows), jnp.float32),
            dma((SLOTS,)), dma((EARLY,)), dma((2,)),
            dma((2, n - 1)), dma((2, n - 1)),
            dma((half - 1,)), dma((half - 1,)),
            dma, dma,
            dma((half - 1,)), dma((half - 1,)),
            dma((n - 1,)), dma((n - 1,)),
            dma((groups,)), dma((groups,)),
            dma((2, n - 1)), dma((2, n - 1)),
        ],
        compiler_params=pltpu.CompilerParams(
            collective_id=0, has_side_effects=True, vmem_limit_bytes=38 * 2**20
        ),
    )(router_weight.T, router_gain[None, :], w_gate, w_up)
    out_gate, out_up, gate_scale, up_scale, router = pl.pallas_call(
        functools.partial(settle, len(held)),
        out_shape=tuple(jax.ShapeDtypeStruct(*a) for a in held),
        in_specs=[vmem] * len(held),
        out_specs=(hbm,) * len(held),
        scratch_shapes=[dma((len(held), PARTS))],
        compiler_params=pltpu.CompilerParams(vmem_limit_bytes=2**20),
    )(*arrived)
    return (
        out_gate.swapaxes(1, 2),
        out_up.swapaxes(1, 2),
        gate_scale,
        up_scale,
        router.T,
    )


def solution(mesh):
    placed = (
        P("expert", "shard", None),
        P("expert", "shard", None),
        P("shard", "expert"),
        P("shard"),
    )
    return jax.shard_map(
        on_device,
        mesh=mesh,
        in_specs=placed,
        out_specs=(
            P("expert", None, "shard"),
            P("expert", None, "shard"),
            P("expert", "shard"),
            P("expert", "shard"),
            P(),
        ),
        check_vma=False,
    )
```

```python
import functools

import jax
import jax.numpy as jnp
from jax import lax
from jax.experimental import pallas as pl
from jax.experimental.pallas import tpu as pltpu
from jax.sharding import PartitionSpec as P

LANES = 128
SLOTS = 4
EARLY = 3
AHEAD = 2
PARTS = 8
LEAD = 3
HELD = 3


def plain(w_gate, w_up, router_weight, router_gain):
    model = w_gate.shape[1] * lax.axis_size("shard")
    total_gate, total_up = lax.psum(
        (jnp.sum(jnp.abs(w_gate), axis=1), jnp.sum(jnp.abs(w_up), axis=1)), "shard"
    )
    served = []
    scales = []
    for w, total in ((w_gate, total_gate), (w_up, total_up)):
        scale = total / model
        narrow = (w / jnp.expand_dims(scale, 1)).astype(jnp.bfloat16)
        out = lax.all_to_all(narrow, "shard", split_axis=2, concat_axis=1, tiled=True)
        served.append(out)
        scales.append(
            lax.dynamic_slice_in_dim(
                scale, lax.axis_index("shard") * out.shape[2], out.shape[2], axis=1
            )
        )
    part_router = (router_weight * router_gain[:, None]).astype(jnp.bfloat16)
    row_router = lax.all_gather(part_router, "shard", axis=0, tiled=True)
    serve_router = lax.all_gather(row_router, "expert", axis=1, tiled=True)
    return (*served, *scales, serve_router)


def kernel(
    n, groups, model,
    weight_ref, gain_ref, gate_ref, up_ref,
    out_gate, out_up, gate_scale, up_scale, out_router, out_held,
    scale_ref, stage, kept, loaded, part, quick, first, near_sum, far_sum, half_sum, raw, gains,
    load_sem, kept_sem, raw_sem, early_send, early_recv,
    near_send, near_recv, far_send, far_recv, mean_send, mean_recv,
    row_send, row_recv, col_send, col_recv, data_send, data_recv, held_sem,
):
    me = lax.axis_index("shard")
    group = lax.axis_index("expert")
    experts, rows, width = gate_ref.shape
    tasks, tiles, _ = part.shape
    half = n // 2
    share = tasks // half
    columns = width // n
    heads = weight_ref.shape[0]
    later = tasks - EARLY
    side, spot = me // half, lax.rem(me, half)

    peers = range(n - 1)
    near = range(half - 1)

    def sent_to(i):
        return lax.rem(me + i + 1, n)

    def come_from(i):
        return lax.rem(me + n - i - 1, n)

    def beside(i):
        return side * half + lax.rem(spot + i + 1, half)

    across = lax.rem(me + half, n)

    def remote(src, dst, send, recv, shard=None, expert=None):
        return pltpu.make_async_remote_copy(
            src_ref=src, dst_ref=dst, send_sem=send, recv_sem=recv,
            device_id={"shard": shard} if expert is None else {"expert": expert},
        )

    def start_load(j):
        task, slot = EARLY + lax.rem(j, later), lax.rem(j, SLOTS)

        @pl.when((j < 2 * later) & (task < experts))
        def _():
            pltpu.make_async_copy(
                gate_ref.at[task], loaded.at[slot], load_sem.at[slot]
            ).start()

        @pl.when((j < 2 * later) & (task >= experts))
        def _():
            pltpu.make_async_copy(
                up_ref.at[task - experts], loaded.at[slot], load_sem.at[slot]
            ).start()

    def wait_load(slot):
        pltpu.make_async_copy(
            gate_ref.at[0], loaded.at[slot], load_sem.at[slot]
        ).wait()

    def keep(task):
        return pltpu.make_async_copy(
            gate_ref.at[task], kept.at[task], kept_sem.at[task]
        )

    def add_up(task, ref, slot):
        for t in range(tiles):
            lanes = slice(t * LANES, (t + 1) * LANES)
            part[task, t : t + 1, :] = jnp.sum(
                jnp.abs(ref[slot, :, lanes]), axis=0, keepdims=True
            )

    def add_later(j, carry):
        slot = lax.rem(j, SLOTS)
        wait_load(slot)
        add_up(EARLY + j, loaded, slot)
        start_load(j + SLOTS)
        return carry

    def shape_task(task, ref, slot, means, index):
        for t in range(tiles):
            lanes = slice(t * LANES, (t + 1) * LANES)
            inverse = 1.0 / means[index, t : t + 1, :]
            scaled = ref[slot, :, lanes] * inverse
            stage[task, lanes, :] = scaled.T.astype(jnp.bfloat16)

    my_rows = pl.ds(pl.multiple_of(me * rows, rows), rows)

    def piece(k):
        return pl.ds(pl.multiple_of(k * columns, 16), columns)

    def send_task(task, w, out, chosen):
        e = task - w * experts
        for i in chosen:
            remote(
                stage.at[task, piece(sent_to(i))],
                out.at[e, :, my_rows],
                data_send.at[w, i],
                data_recv.at[w, i],
                shard=sent_to(i),
            ).start()

    def keep_own(task, w, out):
        out[task - w * experts, :, my_rows] = stage[task, piece(me)]

    for task in range(EARLY):
        keep(task).start()
    fetch_weight = pltpu.make_async_copy(weight_ref, raw, raw_sem.at[0])
    fetch_gain = pltpu.make_async_copy(gain_ref, gains, raw_sem.at[1])
    fetch_weight.start()
    fetch_gain.start()
    for j in range(SLOTS):
        start_load(j)

    barrier = pltpu.get_barrier_semaphore()
    for i in peers:
        pl.semaphore_signal(barrier, inc=1, device_id={"shard": sent_to(i)})
    for q in range(1, groups):
        pl.semaphore_signal(
            barrier, inc=1, device_id={"expert": lax.rem(group + q, groups)}
        )

    started = []

    def begin(copy):
        copy.start()
        started.append(copy)
        return copy

    keep(0).wait()
    add_up(0, kept, 0)
    pl.semaphore_wait(barrier, n - 1 + groups - 1)

    early = []
    for i in peers:
        early.append(begin(remote(
            part.at[pl.ds(0, 1)], first.at[me, pl.ds(0, 1)],
            early_send.at[0, i], early_recv.at[0, i], shard=sent_to(i),
        )))
    first[me, 0:1] = part[0:1]
    for task in range(1, EARLY):
        keep(task).wait()
        add_up(task, kept, task)
    rest = []
    for i in peers:
        rest.append(begin(remote(
            part.at[pl.ds(1, EARLY - 1)], first.at[me, pl.ds(1, EARLY - 1)],
            early_send.at[1, i], early_recv.at[1, i], shard=sent_to(i),
        )))
    first[me, 1:EARLY] = part[1:EARLY]

    fetch_weight.wait()
    fetch_gain.wait()
    mine = pl.ds(pl.multiple_of(group * heads, heads), heads)
    out_router[mine, my_rows] = (raw[...] * gains[...]).astype(jnp.bfloat16)
    lines = []
    for i in peers:
        lines.append(begin(remote(
            out_router.at[mine, my_rows], out_router.at[mine, my_rows],
            row_send.at[i], row_recv.at[i], shard=sent_to(i),
        )))

    lax.fori_loop(0, AHEAD, add_later, 0)

    def early_mean(lo, hi):
        total = first[0, lo:hi]
        for s in range(1, n):
            total = total + first[s, lo:hi]
        quick[lo:hi] = total / model

    for copy in early:
        copy.wait_recv()
    early_mean(0, 1)
    shape_task(0, kept, 0, quick, 0)
    send_task(0, 0, out_gate, peers)

    lax.fori_loop(AHEAD, later, add_later, 0)

    sums = []
    for i in near:
        sums.append(begin(remote(
            part.at[pl.ds(lax.rem(beside(i), half) * share, share)],
            near_sum.at[i], near_send.at[i], near_recv.at[i], shard=beside(i),
        )))
    keep_own(0, 0, out_gate)
    for copy in rest:
        copy.wait_recv()
    early_mean(1, EARLY)
    shape_task(1, kept, 1, quick, 1)
    send_task(1, 0, out_gate, range(LEAD))

    own = pl.ds(spot * share, share)
    total = part[own]
    for i, copy in zip(near, sums):
        copy.wait_recv()
        total = total + near_sum[i]
    half_sum[...] = total
    crossing = begin(remote(half_sum, far_sum, far_send, far_recv, shard=across))
    send_task(1, 0, out_gate, range(LEAD, n - 1))
    keep_own(1, 0, out_gate)

    for task in range(2, EARLY):
        shape_task(task, kept, task, quick, task)
    crossing.wait_recv()
    scale_ref[own] = (half_sum[...] + far_sum[...]) / model
    means = []
    for i in near:
        means.append(begin(remote(
            scale_ref.at[own], scale_ref.at[own],
            mean_send.at[i], mean_recv.at[i], shard=beside(i),
        )))
    for task in range(2, EARLY):
        send_task(task, 0, out_gate, peers)
        keep_own(task, 0, out_gate)

    for copy in lines:
        copy.wait_recv()
    cols = []
    for q in range(1, groups):
        cols.append(begin(remote(
            out_router.at[mine], out_router.at[mine],
            col_send.at[q], col_recv.at[q], expert=lax.rem(group + q, groups),
        )))
    for copy in means:
        copy.wait_recv()

    for k in range(n):

        @pl.when(me == k)
        def _(k=k):
            lo = k * columns
            for t in range(lo // LANES, (lo + columns - 1) // LANES + 1):
                left = max(lo, t * LANES)
                right = min(lo + columns, (t + 1) * LANES)
                seen = scale_ref[:, t, left - t * LANES : right - t * LANES]
                gate_scale[:, left - lo : right - lo] = seen[:experts]
                up_scale[:, left - lo : right - lo] = seen[experts:]

    for w, out in enumerate((out_gate, out_up)):

        def step(task, carry, w=w, out=out, chosen=peers):
            j = later + task - EARLY
            slot = lax.rem(j, SLOTS)
            wait_load(slot)
            shape_task(task, loaded, slot, scale_ref, task)
            send_task(task, w, out, chosen)
            keep_own(task, w, out)
            start_load(j + SLOTS)
            return carry

        stop = (w + 1) * experts - (HELD if w else 0)
        lax.fori_loop(max(EARLY, w * experts), stop, step, 0)

    fewer = functools.partial(step, chosen=[i for i in peers if i != half - 1])
    lax.fori_loop(tasks - HELD, tasks, fewer, 0)
    holding = pltpu.make_async_copy(
        stage.at[pl.ds(tasks - HELD, HELD), piece(across)], out_held, held_sem
    )
    holding.start()

    for copy in cols:
        copy.wait_recv()
    for copy in started:
        copy.wait_send()
    for w, out in enumerate((out_gate, out_up)):
        for i in peers:
            count = experts - (HELD if w and i == half - 1 else 0)
            held = pl.ds(w * experts, count)
            from_i = pl.ds(pl.multiple_of(come_from(i) * rows, rows), rows)
            both = remote(
                stage.at[held, piece(sent_to(i))], out.at[pl.ds(0, count), :, from_i],
                data_send.at[w, i], data_recv.at[w, i], shard=sent_to(i),
            )
            both.wait_send()
            both.wait_recv()
    holding.wait()


def place(count, n, up_ref, got_ref, out_ref, sem):
    me = lax.axis_index("shard")
    experts, _, model = up_ref.shape
    rows = model // n
    across = lax.rem(me + n // 2, n)
    there = pl.ds(pl.multiple_of(across * rows, rows), rows)
    copy = pltpu.make_async_copy(
        got_ref, out_ref.at[pl.ds(experts - count, count), :, there], sem
    )
    copy.start()
    copy.wait()


def settle(count, *refs):
    sources, outs, sem = refs[:count], refs[count : 2 * count], refs[-1]
    copies = []
    for i, (src, dst) in enumerate(zip(sources, outs)):
        parts = PARTS if src.ndim == 3 and src.shape[0] % PARTS == 0 else 1
        step = src.shape[0] // parts
        for k in range(parts):
            rows = pl.ds(k * step, step)
            copies.append(
                pltpu.make_async_copy(src.at[rows], dst.at[rows], sem.at[i, k])
            )
    for copy in copies:
        copy.start()
    for copy in copies:
        copy.wait()


def on_device(w_gate, w_up, router_weight, router_gain):
    n, groups = lax.axis_size("shard"), lax.axis_size("expert")
    experts, rows, width = w_gate.shape
    heads = router_weight.shape[1]
    tasks, columns, model = 2 * experts, width // n, rows * n
    if (
        n % 2
        or n < 4
        or rows % LANES
        or width % LANES
        or columns % 16
        or heads % 16
        or tasks % (n // 2)
        or experts < EARLY + AHEAD
    ):
        return plain(w_gate, w_up, router_weight, router_gain)
    tiles, half = width // LANES, n // 2
    share = tasks // half
    hbm = pl.BlockSpec(memory_space=pl.ANY)
    vmem = pl.BlockSpec(memory_space=pltpu.VMEM)
    dma = pltpu.SemaphoreType.DMA
    held = (
        ((experts, columns, model), jnp.bfloat16),
        ((experts, columns, model), jnp.bfloat16),
        ((experts, columns), jnp.float32),
        ((experts, columns), jnp.float32),
        ((heads * groups, model), jnp.bfloat16),
    )
    block = (share, tiles, LANES)
    *arrived, kept_back = pl.pallas_call(
        functools.partial(kernel, n, groups, model),
        out_shape=(
            *(pltpu.VMEM(*a) for a in held),
            jax.ShapeDtypeStruct((HELD, columns, rows), jnp.bfloat16),
        ),
        in_specs=[hbm] * 4,
        out_specs=(vmem,) * len(held) + (hbm,),
        scratch_shapes=[
            pltpu.VMEM((tasks, tiles, LANES), jnp.float32),
            pltpu.VMEM((tasks, width, rows), jnp.bfloat16),
            pltpu.VMEM((EARLY, rows, width), jnp.float32),
            pltpu.VMEM((SLOTS, rows, width), jnp.float32),
            pltpu.VMEM((tasks, tiles, LANES), jnp.float32),
            pltpu.VMEM((EARLY, tiles, LANES), jnp.float32),
            pltpu.VMEM((n, EARLY, tiles, LANES), jnp.float32),
            pltpu.VMEM((half - 1, *block), jnp.float32),
            pltpu.VMEM(block, jnp.float32),
            pltpu.VMEM(block, jnp.float32),
            pltpu.VMEM((heads, rows), jnp.float32),
            pltpu.VMEM((1, rows), jnp.float32),
            dma((SLOTS,)), dma((EARLY,)), dma((2,)),
            dma((2, n - 1)), dma((2, n - 1)),
            dma((half - 1,)), dma((half - 1,)),
            dma, dma,
            dma((half - 1,)), dma((half - 1,)),
            dma((n - 1,)), dma((n - 1,)),
            dma((groups,)), dma((groups,)),
            dma((2, n - 1)), dma((2, n - 1)), dma,
        ],
        compiler_params=pltpu.CompilerParams(
            collective_id=0, has_side_effects=True, vmem_limit_bytes=38 * 2**20
        ),
    )(router_weight.T, router_gain[None, :], w_gate, w_up)
    swapped = lax.ppermute(
        kept_back, "shard", [(s, (s + half) % n) for s in range(n)]
    )
    out_gate, out_up, gate_scale, up_scale, router = pl.pallas_call(
        functools.partial(settle, len(held)),
        out_shape=tuple(jax.ShapeDtypeStruct(*a) for a in held),
        in_specs=[vmem] * len(held),
        out_specs=(hbm,) * len(held),
        scratch_shapes=[dma((len(held), PARTS))],
        cost_estimate=pl.CostEstimate(
            flops=4 * 10**8, bytes_accessed=8 * w_gate.size, transcendentals=0
        ),
        compiler_params=pltpu.CompilerParams(vmem_limit_bytes=2**20),
    )(*arrived)
    out_up = pl.pallas_call(
        functools.partial(place, HELD, n),
        out_shape=jax.ShapeDtypeStruct(out_up.shape, out_up.dtype),
        in_specs=[hbm, hbm],
        out_specs=hbm,
        scratch_shapes=[dma],
        input_output_aliases={0: 0},
        compiler_params=pltpu.CompilerParams(vmem_limit_bytes=2**20),
    )(out_up, swapped)
    return (
        out_gate.swapaxes(1, 2),
        out_up.swapaxes(1, 2),
        gate_scale,
        up_scale,
        router.T,
    )


def solution(mesh):
    placed = (
        P("expert", "shard", None),
        P("expert", "shard", None),
        P("shard", "expert"),
        P("shard"),
    )
    return jax.shard_map(
        on_device,
        mesh=mesh,
        in_specs=placed,
        out_specs=(
            P("expert", None, "shard"),
            P("expert", None, "shard"),
            P("expert", "shard"),
            P("expert", "shard"),
            P(),
        ),
        check_vma=False,
    )
```

```python
import functools

import jax
import jax.numpy as jnp
from jax import lax
from jax.experimental import pallas as pl
from jax.experimental.pallas import tpu as pltpu
from jax.sharding import PartitionSpec as P

LANES = 128
SLOTS = 4
EARLY = 3
AHEAD = 3
PARTS = 8
LEAD = 3
HELD = 3


def plain(w_gate, w_up, router_weight, router_gain):
    model = w_gate.shape[1] * lax.axis_size("shard")
    total_gate, total_up = lax.psum(
        (jnp.sum(jnp.abs(w_gate), axis=1), jnp.sum(jnp.abs(w_up), axis=1)), "shard"
    )
    served = []
    scales = []
    for w, total in ((w_gate, total_gate), (w_up, total_up)):
        scale = total / model
        narrow = (w / jnp.expand_dims(scale, 1)).astype(jnp.bfloat16)
        out = lax.all_to_all(narrow, "shard", split_axis=2, concat_axis=1, tiled=True)
        served.append(out)
        scales.append(
            lax.dynamic_slice_in_dim(
                scale, lax.axis_index("shard") * out.shape[2], out.shape[2], axis=1
            )
        )
    part_router = (router_weight * router_gain[:, None]).astype(jnp.bfloat16)
    row_router = lax.all_gather(part_router, "shard", axis=0, tiled=True)
    serve_router = lax.all_gather(row_router, "expert", axis=1, tiled=True)
    return (*served, *scales, serve_router)


def kernel(
    n, groups, model,
    weight_ref, gain_ref, gate_ref, up_ref,
    out_gate, out_up, gate_scale, up_scale, out_router, out_held,
    scale_ref, stage, kept, loaded, part, quick, first, near_sum, far_sum, half_sum, raw, gains,
    load_sem, kept_sem, raw_sem, early_send, early_recv,
    near_send, near_recv, far_send, far_recv, mean_send, mean_recv,
    row_send, row_recv, col_send, col_recv, data_send, data_recv,
):
    me = lax.axis_index("shard")
    group = lax.axis_index("expert")
    experts, rows, width = gate_ref.shape
    tasks, tiles, _ = part.shape
    half = n // 2
    share = tasks // half
    columns = width // n
    heads = weight_ref.shape[0]
    later = tasks - EARLY
    side, spot = me // half, lax.rem(me, half)

    peers = range(n - 1)
    near = range(half - 1)

    def sent_to(i):
        return lax.rem(me + i + 1, n)

    def come_from(i):
        return lax.rem(me + n - i - 1, n)

    def beside(i):
        return side * half + lax.rem(spot + i + 1, half)

    across = lax.rem(me + half, n)

    def remote(src, dst, send, recv, shard=None, expert=None):
        return pltpu.make_async_remote_copy(
            src_ref=src, dst_ref=dst, send_sem=send, recv_sem=recv,
            device_id={"shard": shard} if expert is None else {"expert": expert},
        )

    def start_load(j):
        task, slot = EARLY + lax.rem(j, later), lax.rem(j, SLOTS)

        @pl.when((j < 2 * later) & (task < experts))
        def _():
            pltpu.make_async_copy(
                gate_ref.at[task], loaded.at[slot], load_sem.at[slot]
            ).start()

        @pl.when((j < 2 * later) & (task >= experts))
        def _():
            pltpu.make_async_copy(
                up_ref.at[task - experts], loaded.at[slot], load_sem.at[slot]
            ).start()

    def wait_load(slot):
        pltpu.make_async_copy(
            gate_ref.at[0], loaded.at[slot], load_sem.at[slot]
        ).wait()

    def keep(task):
        return pltpu.make_async_copy(
            gate_ref.at[task], kept.at[task], kept_sem.at[task]
        )

    def add_up(task, ref, slot):
        for t in range(tiles):
            lanes = slice(t * LANES, (t + 1) * LANES)
            part[task, t : t + 1, :] = jnp.sum(
                jnp.abs(ref[slot, :, lanes]), axis=0, keepdims=True
            )

    def add_later(j, carry):
        slot = lax.rem(j, SLOTS)
        wait_load(slot)
        add_up(EARLY + j, loaded, slot)
        start_load(j + SLOTS)
        return carry

    def shape_task(task, ref, slot, means, index):
        for t in range(tiles):
            lanes = slice(t * LANES, (t + 1) * LANES)
            inverse = 1.0 / means[index, t : t + 1, :]
            scaled = ref[slot, :, lanes] * inverse
            stage[task, lanes, :] = scaled.T.astype(jnp.bfloat16)

    my_rows = pl.ds(pl.multiple_of(me * rows, rows), rows)

    def piece(k):
        return pl.ds(pl.multiple_of(k * columns, 16), columns)

    def send_task(task, w, out, chosen):
        e = task - w * experts
        for i in chosen:
            remote(
                stage.at[task, piece(sent_to(i))],
                out.at[e, :, my_rows],
                data_send.at[w, i],
                data_recv.at[w, i],
                shard=sent_to(i),
            ).start()

    def keep_own(task, w, out):
        out[task - w * experts, :, my_rows] = stage[task, piece(me)]

    keep(0).start()
    fetch_weight = pltpu.make_async_copy(weight_ref, raw, raw_sem.at[0])
    fetch_gain = pltpu.make_async_copy(gain_ref, gains, raw_sem.at[1])

    barrier = pltpu.get_barrier_semaphore()
    for i in peers:
        pl.semaphore_signal(barrier, inc=1, device_id={"shard": sent_to(i)})
    for q in range(1, groups):
        pl.semaphore_signal(
            barrier, inc=1, device_id={"expert": lax.rem(group + q, groups)}
        )

    started = []

    def begin(copy):
        copy.start()
        started.append(copy)
        return copy

    keep(0).wait()
    for task in range(1, EARLY):
        keep(task).start()
    fetch_weight.start()
    fetch_gain.start()
    for j in range(SLOTS):
        start_load(j)
    add_up(0, kept, 0)
    pl.semaphore_wait(barrier, n - 1 + groups - 1)

    early = []
    for i in peers:
        early.append(begin(remote(
            part.at[pl.ds(0, 1)], first.at[me, pl.ds(0, 1)],
            early_send.at[0, i], early_recv.at[0, i], shard=sent_to(i),
        )))
    first[me, 0:1] = part[0:1]
    for task in range(1, EARLY):
        keep(task).wait()
        add_up(task, kept, task)
    rest = []
    for i in peers:
        rest.append(begin(remote(
            part.at[pl.ds(1, EARLY - 1)], first.at[me, pl.ds(1, EARLY - 1)],
            early_send.at[1, i], early_recv.at[1, i], shard=sent_to(i),
        )))
    first[me, 1:EARLY] = part[1:EARLY]

    fetch_weight.wait()
    fetch_gain.wait()
    mine = pl.ds(pl.multiple_of(group * heads, heads), heads)
    out_router[mine, my_rows] = (raw[...] * gains[...]).astype(jnp.bfloat16)
    lines = []
    for i in peers:
        lines.append(begin(remote(
            out_router.at[mine, my_rows], out_router.at[mine, my_rows],
            row_send.at[i], row_recv.at[i], shard=sent_to(i),
        )))

    lax.fori_loop(0, AHEAD, add_later, 0)

    def early_mean(lo, hi):
        total = first[0, lo:hi]
        for s in range(1, n):
            total = total + first[s, lo:hi]
        quick[lo:hi] = total / model

    for copy in early:
        copy.wait_recv()
    early_mean(0, 1)
    shape_task(0, kept, 0, quick, 0)
    send_task(0, 0, out_gate, peers)

    lax.fori_loop(AHEAD, later, add_later, 0)

    sums = []
    for i in near:
        sums.append(begin(remote(
            part.at[pl.ds(lax.rem(beside(i), half) * share, share)],
            near_sum.at[i], near_send.at[i], near_recv.at[i], shard=beside(i),
        )))
    keep_own(0, 0, out_gate)
    for copy in rest:
        copy.wait_recv()
    early_mean(1, EARLY)
    shape_task(1, kept, 1, quick, 1)
    send_task(1, 0, out_gate, range(LEAD))

    own = pl.ds(spot * share, share)
    total = part[own]
    for i, copy in zip(near, sums):
        copy.wait_recv()
        total = total + near_sum[i]
    half_sum[...] = total
    crossing = begin(remote(half_sum, far_sum, far_send, far_recv, shard=across))
    send_task(1, 0, out_gate, range(LEAD, n - 1))
    keep_own(1, 0, out_gate)

    for task in range(2, EARLY):
        shape_task(task, kept, task, quick, task)
    crossing.wait_recv()
    scale_ref[own] = (half_sum[...] + far_sum[...]) / model
    means = []
    for i in near:
        means.append(begin(remote(
            scale_ref.at[own], scale_ref.at[own],
            mean_send.at[i], mean_recv.at[i], shard=beside(i),
        )))
    for task in range(2, EARLY):
        send_task(task, 0, out_gate, peers)
        keep_own(task, 0, out_gate)

    for copy in lines:
        copy.wait_recv()
    cols = []
    for q in range(1, groups):
        cols.append(begin(remote(
            out_router.at[mine], out_router.at[mine],
            col_send.at[q], col_recv.at[q], expert=lax.rem(group + q, groups),
        )))
    for copy in means:
        copy.wait_recv()

    for k in range(n):

        @pl.when(me == k)
        def _(k=k):
            lo = k * columns
            for t in range(lo // LANES, (lo + columns - 1) // LANES + 1):
                left = max(lo, t * LANES)
                right = min(lo + columns, (t + 1) * LANES)
                seen = scale_ref[:, t, left - t * LANES : right - t * LANES]
                gate_scale[:, left - lo : right - lo] = seen[:experts]
                up_scale[:, left - lo : right - lo] = seen[experts:]

    for w, out in enumerate((out_gate, out_up)):

        def step(task, carry, w=w, out=out, chosen=peers):
            j = later + task - EARLY
            slot = lax.rem(j, SLOTS)
            wait_load(slot)
            shape_task(task, loaded, slot, scale_ref, task)
            send_task(task, w, out, chosen)
            keep_own(task, w, out)
            start_load(j + SLOTS)
            return carry

        stop = (w + 1) * experts - (HELD if w else 0)
        lax.fori_loop(max(EARLY, w * experts), stop, step, 0)

    fewer = functools.partial(step, chosen=[i for i in peers if i != half - 1])
    lax.fori_loop(tasks - HELD, tasks, fewer, 0)
    out_held[...] = stage[pl.ds(tasks - HELD, HELD), piece(across)]

    for copy in cols:
        copy.wait_recv()
    for copy in started:
        copy.wait_send()
    for w, out in enumerate((out_gate, out_up)):
        for i in peers:
            count = experts - (HELD if w and i == half - 1 else 0)
            held = pl.ds(w * experts, count)
            from_i = pl.ds(pl.multiple_of(come_from(i) * rows, rows), rows)
            both = remote(
                stage.at[held, piece(sent_to(i))], out.at[pl.ds(0, count), :, from_i],
                data_send.at[w, i], data_recv.at[w, i], shard=sent_to(i),
            )
            both.wait_send()
            both.wait_recv()


def place(count, n, up_ref, got_ref, out_ref, sem):
    me = lax.axis_index("shard")
    experts, _, model = up_ref.shape
    rows = model // n
    across = lax.rem(me + n // 2, n)
    there = pl.ds(pl.multiple_of(across * rows, rows), rows)
    copy = pltpu.make_async_copy(
        got_ref, out_ref.at[pl.ds(experts - count, count), :, there], sem
    )
    copy.start()
    copy.wait()


def settle(count, *refs):
    sources, outs, sem = refs[:count], refs[count : 2 * count], refs[-1]
    copies = []
    for i, (src, dst) in enumerate(zip(sources, outs)):
        parts = PARTS if src.ndim == 3 and src.shape[0] % PARTS == 0 else 1
        step = src.shape[0] // parts
        for k in range(parts):
            rows = pl.ds(k * step, step)
            copies.append(
                pltpu.make_async_copy(src.at[rows], dst.at[rows], sem.at[i, k])
            )
    for copy in copies:
        copy.start()
    for copy in copies:
        copy.wait()


def on_device(w_gate, w_up, router_weight, router_gain):
    n, groups = lax.axis_size("shard"), lax.axis_size("expert")
    experts, rows, width = w_gate.shape
    heads = router_weight.shape[1]
    tasks, columns, model = 2 * experts, width // n, rows * n
    if (
        n % 2
        or n < 4
        or rows % LANES
        or width % LANES
        or columns % 16
        or heads % 16
        or tasks % (n // 2)
        or experts < EARLY + AHEAD
    ):
        return plain(w_gate, w_up, router_weight, router_gain)
    tiles, half = width // LANES, n // 2
    share = tasks // half
    hbm = pl.BlockSpec(memory_space=pl.ANY)
    vmem = pl.BlockSpec(memory_space=pltpu.VMEM)
    dma = pltpu.SemaphoreType.DMA
    held = (
        ((experts, columns, model), jnp.bfloat16),
        ((experts, columns, model), jnp.bfloat16),
        ((experts, columns), jnp.float32),
        ((experts, columns), jnp.float32),
        ((heads * groups, model), jnp.bfloat16),
    )
    block = (share, tiles, LANES)
    *arrived, kept_back = pl.pallas_call(
        functools.partial(kernel, n, groups, model),
        out_shape=(
            *(pltpu.VMEM(*a) for a in held),
            pltpu.VMEM((HELD, columns, rows), jnp.bfloat16),
        ),
        in_specs=[hbm] * 4,
        out_specs=(vmem,) * (len(held) + 1),
        scratch_shapes=[
            pltpu.VMEM((tasks, tiles, LANES), jnp.float32),
            pltpu.VMEM((tasks, width, rows), jnp.bfloat16),
            pltpu.VMEM((EARLY, rows, width), jnp.float32),
            pltpu.VMEM((SLOTS, rows, width), jnp.float32),
            pltpu.VMEM((tasks, tiles, LANES), jnp.float32),
            pltpu.VMEM((EARLY, tiles, LANES), jnp.float32),
            pltpu.VMEM((n, EARLY, tiles, LANES), jnp.float32),
            pltpu.VMEM((half - 1, *block), jnp.float32),
            pltpu.VMEM(block, jnp.float32),
            pltpu.VMEM(block, jnp.float32),
            pltpu.VMEM((heads, rows), jnp.float32),
            pltpu.VMEM((1, rows), jnp.float32),
            dma((SLOTS,)), dma((EARLY,)), dma((2,)),
            dma((2, n - 1)), dma((2, n - 1)),
            dma((half - 1,)), dma((half - 1,)),
            dma, dma,
            dma((half - 1,)), dma((half - 1,)),
            dma((n - 1,)), dma((n - 1,)),
            dma((groups,)), dma((groups,)),
            dma((2, n - 1)), dma((2, n - 1)),
        ],
        compiler_params=pltpu.CompilerParams(
            collective_id=0, has_side_effects=True, vmem_limit_bytes=38 * 2**20
        ),
    )(router_weight.T, router_gain[None, :], w_gate, w_up)
    swapped = lax.ppermute(
        kept_back, "shard", [(s, (s + half) % n) for s in range(n)]
    )
    out_gate, out_up, gate_scale, up_scale, router = pl.pallas_call(
        functools.partial(settle, len(held)),
        out_shape=tuple(jax.ShapeDtypeStruct(*a) for a in held),
        in_specs=[vmem] * len(held),
        out_specs=(hbm,) * len(held),
        scratch_shapes=[dma((len(held), PARTS))],
        cost_estimate=pl.CostEstimate(
            flops=4 * 10**8, bytes_accessed=8 * w_gate.size, transcendentals=0
        ),
        compiler_params=pltpu.CompilerParams(vmem_limit_bytes=2**20),
    )(*arrived)
    out_up = pl.pallas_call(
        functools.partial(place, HELD, n),
        out_shape=jax.ShapeDtypeStruct(out_up.shape, out_up.dtype),
        in_specs=[hbm, hbm],
        out_specs=hbm,
        scratch_shapes=[dma],
        input_output_aliases={0: 0},
        compiler_params=pltpu.CompilerParams(vmem_limit_bytes=2**20),
    )(out_up, swapped)
    return (
        out_gate.swapaxes(1, 2),
        out_up.swapaxes(1, 2),
        gate_scale,
        up_scale,
        router.T,
    )


def solution(mesh):
    placed = (
        P("expert", "shard", None),
        P("expert", "shard", None),
        P("shard", "expert"),
        P("shard"),
    )
    return jax.shard_map(
        on_device,
        mesh=mesh,
        in_specs=placed,
        out_specs=(
            P("expert", None, "shard"),
            P("expert", None, "shard"),
            P("expert", "shard"),
            P("expert", "shard"),
            P(),
        ),
        check_vma=False,
    )
```
